16 devices in a mesh: dp: 2 (over y, z), cp: 8 (over x, core).
Axes of the slice: x: 4, y: 2, z: 1, core: 2. Of those that a mesh axis runs over, the one named last changes fastest.
The devices are a block of a 4x4x8 slice.
Arguments:
- x_act: bfloat16 [8192, 2048], P(('dp', 'cp')), parts along dimension 0
- seg_ids: int32 [8192], P(('dp', 'cp')), parts along dimension 0
- w_q: bfloat16 [2048, 16, 128], replicated
- w_k: bfloat16 [2048, 2, 128], replicated
- w_v: bfloat16 [2048, 2, 128], replicated
- w_o: bfloat16 [2048, 16, 128], replicated
- dy_act: bfloat16 [8192, 2048], P(('dp', 'cp')), parts along dimension 0
Outputs:
- output 1: bfloat16 [8192, 2048], P(('dp', 'cp')), parts along dimension 0
- output 2: bfloat16 [8192, 2048], P(('dp', 'cp')), parts along dimension 0
- output 3: float32 [4096, 16, 128], P(('dp', 'cp')), parts along dimension 0
- output 4: float32 [4096, 2, 128], P(('dp', 'cp')), parts along dimension 0
- output 5: float32 [4096, 2, 128], P(('dp', 'cp')), parts along dimension 0
- output 6: float32 [4096, 16, 128], P(('dp', 'cp')), parts along dimension 0
There are 2 independent parts. The reference program is written for one: setup_inputs(seed, part) draws one part's arguments, and reference() takes and returns one part's arrays. A program takes and returns all parts, laid end to end along the dimension named above; an argument that names none is the same for every part.
All inputs are finite; a program needn't handle non-finite values.
Results may differ from the reference program's by a relative error of at most 0.02.
Values are sent between devices in bfloat16 or wider.
A program may use at most 768 MiB of HBM per device.

```python
import jax
import jax.numpy as jnp
from jax import lax

CP_SIZE = 8
TOK_DEV = 512
MODEL_DIM = 2048
Q_HEADS = 16
KV_HEADS = 2
HEAD_DIM = 128

SEQ_LEN = CP_SIZE * TOK_DEV
GROUP_SIZE = Q_HEADS // KV_HEADS
Q_BLOCK = min(TOK_DEV, 128)
N_BLOCKS = SEQ_LEN // Q_BLOCK


def draw_segments(seg_key):
    key_zone, key_kind, key_short = jax.random.split(seg_key, 3)
    positions = jnp.arange(SEQ_LEN)
    zone_start = (jax.random.randint(key_zone, (SEQ_LEN,), 0, 2 * TOK_DEV) == 0) | (positions == 0)
    zone_index = jnp.cumsum(zone_start.astype(jnp.int32))
    parity = jax.random.randint(key_kind, (), 0, 2)
    short_zone = (zone_index + parity) % 2 == 0
    short_start = jax.random.randint(key_short, (SEQ_LEN,), 0, max(TOK_DEV // 8, 2)) == 0
    starts = zone_start | (short_zone & short_start)
    return (jnp.cumsum(starts.astype(jnp.int32)) - 1).astype(jnp.int32)


def setup_inputs(seed: int = 0, part: int = 0) -> dict:
    base_key = jax.random.key(seed)
    part_key = jax.random.fold_in(base_key, part)
    weight_key = jax.random.fold_in(base_key, 1000003)
    key_seg, key_x, key_dy = jax.random.split(part_key, 3)
    key_q, key_k, key_v, key_o = jax.random.split(weight_key, 4)
    in_scale = MODEL_DIM ** -0.5
    out_scale = (Q_HEADS * HEAD_DIM) ** -0.5
    q_shape = (MODEL_DIM, Q_HEADS, HEAD_DIM)
    kv_shape = (MODEL_DIM, KV_HEADS, HEAD_DIM)
    return {
        'x_act': jax.random.normal(key_x, (SEQ_LEN, MODEL_DIM), jnp.float32).astype(jnp.bfloat16),
        'seg_ids': draw_segments(key_seg),
        'w_q': (1.5 * in_scale * jax.random.normal(key_q, q_shape, jnp.float32)).astype(jnp.bfloat16),
        'w_k': (in_scale * jax.random.normal(key_k, kv_shape, jnp.float32)).astype(jnp.bfloat16),
        'w_v': (in_scale * jax.random.normal(key_v, kv_shape, jnp.float32)).astype(jnp.bfloat16),
        'w_o': (out_scale * jax.random.normal(key_o, q_shape, jnp.float32)).astype(jnp.bfloat16),
        'dy_act': jax.random.normal(key_dy, (SEQ_LEN, MODEL_DIM), jnp.float32).astype(jnp.bfloat16),
    }


def product32(einsum_form, left_arg, right_arg):
    return jnp.einsum(einsum_form, left_arg.astype(jnp.float32), right_arg.astype(jnp.float32))


def reference(x_act, seg_ids, w_q, w_k, w_v, w_o, dy_act):
    score_scale = HEAD_DIM ** -0.5
    w_q4 = w_q.reshape(MODEL_DIM, KV_HEADS, GROUP_SIZE, HEAD_DIM)
    w_o4 = w_o.reshape(MODEL_DIM, KV_HEADS, GROUP_SIZE, HEAD_DIM)
    q_all = product32('sm,mkgd->skgd', x_act, w_q4).astype(jnp.bfloat16)
    k_all = product32('sm,mkd->skd', x_act, w_k).astype(jnp.bfloat16)
    v_all = product32('sm,mkd->skd', x_act, w_v).astype(jnp.bfloat16)
    do_all = product32('qm,mkgd->qkgd', dy_act, w_o4).astype(jnp.bfloat16)
    k_wide = k_all.astype(jnp.float32)
    v_wide = v_all.astype(jnp.float32)
    key_pos = jnp.arange(SEQ_LEN)

    def block_step(carry_in, block_in):
        dk_acc, dv_acc = carry_in
        q_blk, do_blk, seg_blk, first_pos = block_in
        q_wide = q_blk.astype(jnp.float32)
        do_wide = do_blk.astype(jnp.float32)
        query_pos = first_pos + jnp.arange(Q_BLOCK)
        allowed = (seg_blk[:, None] == seg_ids[None, :]) & (key_pos[None, :] <= query_pos[:, None])
        scores = jnp.einsum('qkgd,skd->kqgs', q_wide, k_wide) * score_scale
        scores = jnp.where(allowed[None, :, None, :], scores, -jnp.inf)
        attn_prob = jax.nn.softmax(scores, axis=-1)
        prob_half = attn_prob.astype(jnp.bfloat16).astype(jnp.float32)
        out_blk = jnp.einsum('kqgs,skd->kqgd', prob_half, v_wide).astype(jnp.bfloat16)
        row_delta = jnp.einsum('qkgd,kqgd->kqg', do_wide, out_blk.astype(jnp.float32))
        dprobs = jnp.einsum('qkgd,skd->kqgs', do_wide, v_wide)
        dscores = (attn_prob * (dprobs - row_delta[..., None])).astype(jnp.bfloat16).astype(jnp.float32)
        dq_blk = (jnp.einsum('kqgs,skd->kqgd', dscores, k_wide) * score_scale).astype(jnp.bfloat16)
        dk_acc = dk_acc + jnp.einsum('kqgs,qkgd->skd', dscores, q_wide)
        dv_acc = dv_acc + jnp.einsum('kqgs,qkgd->skd', prob_half, do_wide)
        return (dk_acc, dv_acc), (out_blk, dq_blk)

    zeros_kv = jnp.zeros((SEQ_LEN, KV_HEADS, HEAD_DIM), jnp.float32)
    block_inputs = (
        q_all.reshape(N_BLOCKS, Q_BLOCK, KV_HEADS, GROUP_SIZE, HEAD_DIM),
        do_all.reshape(N_BLOCKS, Q_BLOCK, KV_HEADS, GROUP_SIZE, HEAD_DIM),
        seg_ids.reshape(N_BLOCKS, Q_BLOCK),
        jnp.arange(N_BLOCKS) * Q_BLOCK,
    )
    (dk_acc, dv_acc), (out_blocks, dq_blocks) = lax.scan(block_step, (zeros_kv, zeros_kv), block_inputs)
    grad_k = (dk_acc * score_scale).astype(jnp.bfloat16)
    grad_v = dv_acc.astype(jnp.bfloat16)
    x_blocks = x_act.reshape(N_BLOCKS, Q_BLOCK, MODEL_DIM)
    dy_blocks = dy_act.reshape(N_BLOCKS, Q_BLOCK, MODEL_DIM)
    y_out = product32('nkqgd,mkgd->nqm', out_blocks, w_o4).reshape(SEQ_LEN, MODEL_DIM).astype(jnp.bfloat16)
    dx_wide = (product32('nkqgd,mkgd->nqm', dq_blocks, w_q4).reshape(SEQ_LEN, MODEL_DIM)
               + product32('skd,mkd->sm', grad_k, w_k) + product32('skd,mkd->sm', grad_v, w_v))
    dx_out = dx_wide.astype(jnp.bfloat16)
    dw_q = product32('nqm,nkqgd->mkgd', x_blocks, dq_blocks).reshape(MODEL_DIM, Q_HEADS, HEAD_DIM)
    dw_k = product32('sm,skd->mkd', x_act, grad_k)
    dw_v = product32('sm,skd->mkd', x_act, grad_v)
    dw_o = product32('nqm,nkqgd->mkgd', dy_blocks, out_blocks).reshape(MODEL_DIM, Q_HEADS, HEAD_DIM)
    return (y_out, dx_out, dw_q, dw_k, dw_v, dw_o)
```

```python
import functools
import jax
import jax.numpy as jnp
from jax import lax
from jax.experimental import pallas as pl
from jax.experimental.pallas import tpu as pltpu
from jax.sharding import PartitionSpec as P

LOG2E = 1.4426950408889634
NEG_START = -1e30
KEY_TILE = 256
HEAD_UNROLL = 4
NT = (((1,), (1,)), ((), ()))
NN = (((1,), (0,)), ((), ()))


def dot32(a, b, dims):
    return lax.dot_general(a, b, dims, preferred_element_type=jnp.float32)


def tile_bias(first_key, n_keys, doc_start, query_pos):
    key_pos = first_key + lax.broadcasted_iota(jnp.int32, (n_keys, doc_start.shape[1]), 0)
    allowed = (key_pos >= doc_start) & (key_pos <= query_pos)
    return jnp.where(allowed, 0.0, -jnp.inf)


def fwd_kernel(scale, meta_ref, start_ref, q_ref, k_ref, v_ref, o_ref, lse_ref, acc_ref, max_ref, sum_ref):
    heads, toks, dim = q_ref.shape
    per_shard = toks // KEY_TILE
    own_tile = meta_ref[1]
    q_first = own_tile * KEY_TILE
    acc_ref[...] = jnp.zeros_like(acc_ref)
    max_ref[...] = jnp.full_like(max_ref, NEG_START)
    sum_ref[...] = jnp.zeros_like(sum_ref)
    coef = scale * LOG2E

    def tile(index, lo):
        shard = index // per_shard
        row = pl.multiple_of((index % per_shard) * KEY_TILE, KEY_TILE)
        keys = k_ref[shard, 0, pl.ds(row, KEY_TILE), :]
        vals_t = v_ref[shard, 0, pl.ds(row, KEY_TILE), :].T
        query_pos = q_first + lo + lax.broadcasted_iota(jnp.int32, (1, toks - lo), 1)
        bias = tile_bias(index * KEY_TILE, KEY_TILE, start_ref[:, lo:], query_pos)
        for h in range(heads):
            scores = dot32(keys, q_ref[h, lo:, :], NT) * coef + bias
            old_max = max_ref[h, :, lo:]
            new_max = jnp.maximum(old_max, jnp.max(scores, axis=0, keepdims=True))
            weights = jnp.exp2(scores - new_max)
            factor = jnp.exp2(old_max - new_max)
            max_ref[h, :, lo:] = new_max
            sum_ref[h, :, lo:] = sum_ref[h, :, lo:] * factor + jnp.sum(weights, axis=0, keepdims=True)
            acc_ref[h, :, lo:] = acc_ref[h, :, lo:] * factor + dot32(vals_t, weights.astype(jnp.bfloat16), NN)

    @pl.loop(meta_ref[0], own_tile + 1)
    def _(index):
        tile(index, 0)

    for extra in range(1, per_shard):
        tile(own_tile + extra, extra * KEY_TILE)
    for h in range(heads):
        o_ref[h] = (acc_ref[h] / sum_ref[h]).T.astype(o_ref.dtype)
        lse_ref[h] = max_ref[h] + jnp.log2(sum_ref[h])


def bwd_kernel(scale, meta_ref, start_ref, q_ref, do_ref, o_ref, lse_ref, k_ref, v_ref, dq_ref, dkv_ref, dqt_ref, delta_ref):
    heads, toks, dim = q_ref.shape
    per_shard = toks // KEY_TILE
    own_tile = meta_ref[1]
    q_first = own_tile * KEY_TILE
    coef = scale * LOG2E

    @pl.when(pl.program_id(1) == 0)
    def _():
        dkv_ref[...] = jnp.zeros_like(dkv_ref)

    dqt_ref[...] = jnp.zeros_like(dqt_ref)
    for h in range(heads):
        prod = do_ref[h].astype(jnp.float32) * o_ref[h].astype(jnp.float32)
        delta_ref[h] = jnp.sum(prod.T, axis=0, keepdims=True)

    def tile(index, lo):
        shard = index // per_shard
        row = pl.multiple_of((index % per_shard) * KEY_TILE, KEY_TILE)
        rows = pl.ds(row, KEY_TILE)
        keys = k_ref[shard, 0, rows, :]
        keys_t = keys.T
        vals = v_ref[shard, 0, rows, :]
        query_pos = q_first + lo + lax.broadcasted_iota(jnp.int32, (1, toks - lo), 1)
        bias = tile_bias(index * KEY_TILE, KEY_TILE, start_ref[:, lo:], query_pos)
        dk = jnp.zeros((KEY_TILE, dim), jnp.float32)
        dv = jnp.zeros((KEY_TILE, dim), jnp.float32)
        for h in range(heads):
            q_h = q_ref[h, lo:, :]
            do_h = do_ref[h, lo:, :]
            scores = dot32(keys, q_h, NT) * coef + bias
            prob = jnp.exp2(scores - lse_ref[h, :, lo:])
            dprob = dot32(vals, do_h, NT)
            dscore = (prob * (dprob - delta_ref[h, :, lo:])).astype(jnp.bfloat16)
            dv = dv + dot32(prob.astype(jnp.bfloat16), do_h, NN)
            dk = dk + dot32(dscore, q_h, NN)
            dqt_ref[h, :, lo:] += dot32(keys_t, dscore, NN)
        dkv_ref[shard, 0, 0, rows, :] += dk
        dkv_ref[shard, 0, 1, rows, :] += dv

    @pl.loop(meta_ref[0], own_tile + 1)
    def _(index):
        tile(index, 0)

    for extra in range(1, per_shard):
        tile(own_tile + extra, extra * KEY_TILE)
    for h in range(heads):
        dq_ref[h] = (dqt_ref[h] * scale).T.astype(dq_ref.dtype)


def tail_kernel(scale, kv_heads, ring, x_ref, gq_ref, dkvp_ref, dwq_ref, dwkv_ref, dkv_ref,
                xp_ref, gqp_ref, xt_ref, w_buf, d_buf, dp_buf, v_buf, bufb_ref, bufp_ref,
                d_load, pair_send, pair_recv, ring_send, ring_recv):
    n = 2 * ring
    idx = lax.axis_index('cp')
    core, chip = idx % 2, idx // 2
    partner = idx + 1 - 2 * core
    hop = ((idx + 2) % n, (idx + n - 2) % n)
    toks, model = x_ref.shape
    heads, _, dim = gq_ref.shape
    rows = model // n
    wide = w_buf.shape[-1]
    per = wide // dim
    parts = w_buf.shape[1]

    def target(way, step):
        return (chip + ring - 1 - step) % ring if way == 0 else (chip + 1 + step) % ring

    barrier = pltpu.get_barrier_semaphore()
    for other in (partner, *hop):
        pl.semaphore_signal(barrier, inc=1, device_id={'cp': other}, device_id_type=pl.DeviceIdType.MESH)

    loads = [[pltpu.make_async_copy(dkvp_ref.at[2 * target(way, step) + core, way], d_buf.at[way, step] if step == 0 else dp_buf.at[1, way, step - 1],
                                    d_load.at[way, step]) for way in range(2)] for step in range(ring)]
    for row in loads:
        for copy in row:
            copy.start()
    pl.semaphore_wait(barrier, 3)

    def to_partner(src, dst, slot):
        return pltpu.make_async_remote_copy(src_ref=src, dst_ref=dst, send_sem=pair_send.at[slot], recv_sem=pair_recv.at[slot],
                                            device_id={'cp': partner}, device_id_type=pl.DeviceIdType.MESH)

    d_pair = [[to_partner(dkvp_ref.at[2 * target(way, step) + 1 - core, way], dp_first(dp_buf, way, step), 2 * step + way)
               for way in range(2)] for step in range(ring)]
    base = 2 * ring
    x_pair = [to_partner(x_ref.at[:, pl.ds(pl.multiple_of((2 * t + 1 - core) * rows, rows), rows)], xp_ref.at[t], base + t) for t in range(ring)]
    q_pair = to_partner(gq_ref, gqp_ref, base + ring)
    b_pair = to_partner(bufb_ref, bufp_ref, base + ring + 1)
    for copy in d_pair[0] + x_pair + [q_pair]:
        copy.start()
    for row in d_pair[1:]:
        for copy in row:
            copy.start()

    class Job:
        def __init__(self, buf, slot, add):
            self.buf, self.slot, self.contribution = buf, slot, add

        def copy(self, way, step):
            return pltpu.make_async_remote_copy(src_ref=self.buf.at[way, step], dst_ref=self.buf.at[way, step + 1],
                                                send_sem=ring_send.at[self.slot, way, step], recv_sem=ring_recv.at[self.slot, way, step],
                                                device_id={'cp': hop[way]}, device_id_type=pl.DeviceIdType.MESH)

        def add(self, step):
            for way in range(2):
                if step:
                    self.copy(way, step - 1).wait_recv()
                self.contribution(way, step)

        def send(self, step):
            for way in range(2):
                self.copy(way, step).start()

        def drain(self):
            for step in range(ring - 1):
                for way in range(2):
                    self.copy(way, step).wait_send()

    def d_add(way, step):
        loads[step][way].wait()
        d_pair[step][way].wait_recv()
        if step == 0:
            d_buf[way, 0] += dp_buf[0, way, 0]
        else:
            d_buf[way, step] += dp_buf[1, way, step - 1] + dp_first(dp_buf, way, step)[...]

    def w_add(part):
        def add(way, step):
            t = target(way, step)
            first = (way * parts + part) * per
            for pair in range(per // 2):
                h = first + 2 * pair
                own = jnp.concatenate([gq_ref[h], gq_ref[h + 1]], axis=1)
                far = jnp.concatenate([gqp_ref[h], gqp_ref[h + 1]], axis=1)
                part_sum = dot32(xt_ref[t, :, :toks], own, NN) + dot32(xt_ref[t, :, toks:], far, NN)
                cols = slice(2 * pair * dim, 2 * (pair + 1) * dim)
                if step == 0:
                    w_buf[way, part, 0, :, cols] = part_sum
                elif step < ring - 1:
                    w_buf[way, part, step, :, cols] += part_sum
                else:
                    dwq_ref[:, h * dim:(h + 2) * dim] = w_buf[way, part, step, :, cols] + part_sum
        return add

    def v_add(way, step):
        t = target(way, step)
        own = jnp.concatenate([bufb_ref[way, g] for g in range(kv_heads)], axis=1)
        far = jnp.concatenate([bufp_ref[way, g] for g in range(kv_heads)], axis=1)
        part_sum = dot32(xt_ref[t, :, :toks], own, NN) + dot32(xt_ref[t, :, toks:], far, NN)
        if step == 0:
            v_buf[way, 0] = part_sum
        elif step < ring - 1:
            v_buf[way, step] += part_sum
        else:
            dwkv_ref[way] = v_buf[way, step] + part_sum

    class Part:
        def __init__(self, part):
            self.part = part

        @property
        def at(self):
            part = self.part

            class View:
                def __getitem__(self, key):
                    return w_buf.at[key[0], part, key[1]]
            return View()

    d_job = Job(d_buf, 0, d_add)
    v_job = Job(v_buf, 1, v_add)
    w_jobs = [Job(Part(part), 2 + part, w_add(part)) for part in range(parts)]

    d_job.add(0)
    d_job.send(0)
    for t in range(ring):
        own_cols = pl.ds(pl.multiple_of((2 * t + core) * rows, rows), rows)
        xt_ref[t, :, :toks] = x_ref[:, own_cols].T
    for t in range(ring):
        x_pair[t].wait_recv()
        xt_ref[t, :, toks:] = xp_ref[t].T
    q_pair.wait_recv()
    w0, w1 = w_jobs
    w0.add(0)
    w0.send(0)
    d_job.add(1)
    d_job.send(1)
    w1.add(0)
    w1.send(0)
    d_job.add(2)
    d_job.send(2)
    for job in w_jobs:
        job.add(1)
        job.send(1)
    d_job.add(ring - 1)
    for g in range(kv_heads):
        bufb_ref[0, g] = (d_buf[g, ring - 1, 0] * scale).astype(bufb_ref.dtype)
        bufb_ref[1, g] = d_buf[g, ring - 1, 1].astype(bufb_ref.dtype)
    dkv_ref[...] = bufb_ref[...]
    b_pair.start()
    b_pair.wait_recv()
    v_job.add(0)
    v_job.send(0)
    w0.add(2)
    w0.send(2)
    v_job.add(1)
    v_job.send(1)
    w1.add(2)
    w1.send(2)
    v_job.add(2)
    v_job.send(2)
    w0.add(3)
    w1.add(3)
    v_job.add(3)
    for copy in [*x_pair, q_pair, b_pair, *sum(d_pair, [])]:
        copy.wait_send()
    for job in (d_job, v_job, *w_jobs):
        job.drain()


def dp_first(dp_buf, way, step):
    return dp_buf.at[0, way, step]


def tail_reduce(x_act, grad_q, dkv_part, scale):
    n, kv_heads, _, toks, dim = dkv_part.shape
    heads, model = grad_q.shape[0], x_act.shape[1]
    ring, rows, parts = n // 2, x_act.shape[1] // n, 2
    wide = heads * dim // (2 * parts)
    bf16, f32 = jnp.bfloat16, jnp.float32
    vmem = pl.BlockSpec(memory_space=pltpu.VMEM)
    n_pair = 3 * ring + 2
    return pl.pallas_call(
        functools.partial(tail_kernel, scale, kv_heads, ring),
        in_specs=[vmem, vmem, pl.BlockSpec(memory_space=pl.ANY)],
        out_specs=[vmem, vmem, vmem],
        out_shape=[jax.ShapeDtypeStruct((rows, heads * dim), f32), jax.ShapeDtypeStruct((2, rows, kv_heads * dim), f32),
                   jax.ShapeDtypeStruct((2, kv_heads, toks, dim), bf16)],
        scratch_shapes=[
            pltpu.VMEM((ring, toks, rows), bf16), pltpu.VMEM((heads, toks, dim), bf16), pltpu.VMEM((ring, rows, 2 * toks), bf16),
            pltpu.VMEM((2, parts, ring, rows, wide), f32), pltpu.VMEM((2, ring, 2, toks, dim), f32),
            pltpu.VMEM((2, 2, ring, 2, toks, dim), f32), pltpu.VMEM((2, ring, rows, kv_heads * dim), f32),
            pltpu.VMEM((2, kv_heads, toks, dim), bf16), pltpu.VMEM((2, kv_heads, toks, dim), bf16),
            pltpu.SemaphoreType.DMA((2, ring)), pltpu.SemaphoreType.DMA((n_pair,)), pltpu.SemaphoreType.DMA((n_pair,)),
            pltpu.SemaphoreType.DMA((2 + parts, 2, ring - 1)), pltpu.SemaphoreType.DMA((2 + parts, 2, ring - 1))],
        compiler_params=pltpu.CompilerParams(collective_id=0, has_side_effects=True, vmem_limit_bytes=56 * 2 ** 20),
        cost_estimate=pl.CostEstimate(flops=2 * 10 ** 11, bytes_accessed=2 ** 24, transcendentals=0),
        name='tail_reduce',
    )(x_act, grad_q, dkv_part)


def solution(mesh):
    group_count = mesh.shape['cp']
    row_spec = P(('dp', 'cp'), None)
    tok_spec = P(('dp', 'cp'))
    weight_spec = P(None, None, None)
    grad_spec = P(('dp', 'cp'), None, None)

    def local_step(x_act, seg_ids, w_q, w_k, w_v, w_o, dy_act):
        toks = x_act.shape[0]
        model_dim, q_heads, dim = w_q.shape
        kv_heads = w_k.shape[1]
        group = q_heads // kv_heads
        halves = group // HEAD_UNROLL
        scale = dim ** -0.5
        my_index = lax.axis_index('cp')
        bf16, f32 = jnp.bfloat16, jnp.float32

        k_loc = jnp.einsum('sm,mkd->ksd', x_act, w_k, preferred_element_type=f32).astype(bf16)
        v_loc = jnp.einsum('sm,mkd->ksd', x_act, w_v, preferred_element_type=f32).astype(bf16)
        kv_all = lax.all_gather(jnp.concatenate([k_loc, v_loc], axis=0), 'cp', axis=0)
        seg_all = lax.all_gather(seg_ids, 'cp', axis=0, tiled=True)
        q_loc = jnp.einsum('sm,mhd->hsd', x_act, w_q, preferred_element_type=f32).astype(bf16)
        do_loc = jnp.einsum('qm,mhd->hqd', dy_act, w_o, preferred_element_type=f32).astype(bf16)
        doc_start = jnp.sum((seg_all[None, :] < seg_ids[:, None]).astype(jnp.int32), axis=1)
        meta = jnp.stack([doc_start[0] // KEY_TILE, my_index * (toks // KEY_TILE)]).astype(jnp.int32)
        start_row = doc_start[None, :]

        grid = (kv_heads, halves)
        head_spec = pl.BlockSpec((HEAD_UNROLL, toks, dim), lambda g, b, m: (g * halves + b, 0, 0))
        stat_spec = pl.BlockSpec((HEAD_UNROLL, 1, toks), lambda g, b, m: (g * halves + b, 0, 0))
        start_spec = pl.BlockSpec((1, toks), lambda g, b, m: (0, 0))
        key_spec = pl.BlockSpec((group_count, 1, toks, dim), lambda g, b, m: (0, g, 0, 0))
        val_spec = pl.BlockSpec((group_count, 1, toks, dim), lambda g, b, m: (0, kv_heads + g, 0, 0))
        tile_flops = 2 * q_heads * toks * toks * dim * 3
        o_loc, lse = pl.pallas_call(
            functools.partial(fwd_kernel, scale),
            grid_spec=pltpu.PrefetchScalarGridSpec(
                num_scalar_prefetch=1, grid=grid,
                in_specs=[start_spec, head_spec, key_spec, val_spec],
                out_specs=[head_spec, stat_spec],
                scratch_shapes=[pltpu.VMEM((HEAD_UNROLL, dim, toks), f32), pltpu.VMEM((HEAD_UNROLL, 1, toks), f32),
                                pltpu.VMEM((HEAD_UNROLL, 1, toks), f32)]),
            out_shape=[jax.ShapeDtypeStruct((q_heads, toks, dim), bf16), jax.ShapeDtypeStruct((q_heads, 1, toks), f32)],
            compiler_params=pltpu.CompilerParams(dimension_semantics=('arbitrary', 'arbitrary'), vmem_limit_bytes=56 * 2 ** 20),
            cost_estimate=pl.CostEstimate(flops=tile_flops * 2, bytes_accessed=2 ** 23, transcendentals=0),
            name='attn_fwd',
        )(meta, start_row, q_loc, kv_all, kv_all)

        def reduce_rows(part_sum):
            return lax.psum_scatter(part_sum, 'cp', scatter_dimension=0, tiled=True)

        dwo_part = jnp.einsum('qm,hqd->mhd', dy_act, o_loc, preferred_element_type=f32)
        dwo = reduce_rows(dwo_part.reshape(model_dim, q_heads * dim)).reshape(-1, q_heads, dim)
        y_out = jnp.einsum('hqd,mhd->qm', o_loc, w_o, preferred_element_type=f32).astype(bf16)

        grad_q, dkv_part = pl.pallas_call(
            functools.partial(bwd_kernel, scale),
            grid_spec=pltpu.PrefetchScalarGridSpec(
                num_scalar_prefetch=1, grid=grid,
                in_specs=[start_spec, head_spec, head_spec, head_spec, stat_spec, key_spec, val_spec],
                out_specs=[head_spec, pl.BlockSpec((group_count, 1, 2, toks, dim), lambda g, b, m: (0, g, 0, 0, 0))],
                scratch_shapes=[pltpu.VMEM((HEAD_UNROLL, dim, toks), f32), pltpu.VMEM((HEAD_UNROLL, 1, toks), f32)]),
            out_shape=[jax.ShapeDtypeStruct((q_heads, toks, dim), bf16),
                       jax.ShapeDtypeStruct((group_count, kv_heads, 2, toks, dim), f32)],
            compiler_params=pltpu.CompilerParams(dimension_semantics=('arbitrary', 'arbitrary'), vmem_limit_bytes=60 * 2 ** 20),
            cost_estimate=pl.CostEstimate(flops=tile_flops * 5, bytes_accessed=2 ** 24, transcendentals=0),
            name='attn_bwd',
        )(meta, start_row, q_loc, do_loc, o_loc, lse, kv_all, kv_all)

        dx_query = jnp.einsum('hqd,mhd->qm', grad_q, w_q, preferred_element_type=f32)
        dwq_rows, dwkv_rows, grad_kv = tail_reduce(x_act, grad_q, dkv_part, scale)
        dwq = dwq_rows.reshape(-1, q_heads, dim)
        dwk, dwv = (dwkv_rows[i].reshape(-1, kv_heads, dim) for i in range(2))
        grad_k, grad_v = grad_kv[0], grad_kv[1]
        dx_wide = (dx_query
                   + jnp.einsum('ksd,mkd->sm', grad_k, w_k, preferred_element_type=f32)
                   + jnp.einsum('ksd,mkd->sm', grad_v, w_v, preferred_element_type=f32))
        return y_out, dx_wide.astype(bf16), dwq, dwk, dwv, dwo

    return jax.shard_map(local_step, mesh=mesh,
                         in_specs=(row_spec, tok_spec, weight_spec, weight_spec, weight_spec, weight_spec, row_spec),
                         out_specs=(row_spec, row_spec, grad_spec, grad_spec, grad_spec, grad_spec),
                         check_vma=False)
```

```python
import functools
import jax
import jax.numpy as jnp
from jax import lax
from jax.experimental import pallas as pl
from jax.experimental.pallas import tpu as pltpu
from jax.sharding import PartitionSpec as P

LOG2E = 1.4426950408889634
NEG_START = -1e30
KEY_TILE = 256
HEAD_UNROLL = 4
BWD_UNROLL = 8
NT = (((1,), (1,)), ((), ()))
NN = (((1,), (0,)), ((), ()))


def dot32(a, b, dims):
    return lax.dot_general(a, b, dims, preferred_element_type=jnp.float32)


def tile_bias(first_key, n_keys, doc_start, query_pos):
    key_pos = first_key + lax.broadcasted_iota(jnp.int32, (n_keys, doc_start.shape[1]), 0)
    allowed = (key_pos >= doc_start) & (key_pos <= query_pos)
    return jnp.where(allowed, 0.0, -jnp.inf)


def fwd_kernel(scale, meta_ref, start_ref, q_ref, k_ref, v_ref, o_ref, lse_ref, acc_ref, max_ref, sum_ref):
    heads, toks, dim = q_ref.shape
    per_shard = toks // KEY_TILE
    own_tile = meta_ref[1]
    q_first = own_tile * KEY_TILE
    acc_ref[...] = jnp.zeros_like(acc_ref)
    max_ref[...] = jnp.full_like(max_ref, NEG_START)
    sum_ref[...] = jnp.zeros_like(sum_ref)
    coef = scale * LOG2E

    def tile(index, size, lo):
        shard = index // per_shard
        row = pl.multiple_of((index % per_shard) * KEY_TILE, KEY_TILE)
        keys = k_ref[shard, 0, 0, pl.ds(row, size), :]
        vals_t = v_ref[shard, 0, 0, pl.ds(row, size), :].T
        query_pos = q_first + lo + lax.broadcasted_iota(jnp.int32, (1, toks - lo), 1)
        bias = tile_bias(index * KEY_TILE, size, start_ref[:, lo:], query_pos)
        for h in range(heads):
            scores = dot32(keys, q_ref[h, lo:, :], NT) * coef + bias
            old_max = max_ref[h, :, lo:]
            new_max = jnp.maximum(old_max, jnp.max(scores, axis=0, keepdims=True))
            weights = jnp.exp2(scores - new_max)
            factor = jnp.exp2(old_max - new_max)
            max_ref[h, :, lo:] = new_max
            sum_ref[h, :, lo:] = sum_ref[h, :, lo:] * factor + jnp.sum(weights, axis=0, keepdims=True)
            acc_ref[h, :, lo:] = acc_ref[h, :, lo:] * factor + dot32(vals_t, weights.astype(jnp.bfloat16), NN)

    first_tile = meta_ref[0]
    odd = jnp.where(first_tile < own_tile, first_tile % per_shard, 0)

    @pl.loop((first_tile + odd) // per_shard, own_tile // per_shard)
    def _(shard):
        tile(shard * per_shard, per_shard * KEY_TILE, 0)

    @pl.loop(0, odd + 1)
    def _(i):
        tile(jnp.where(i < odd, first_tile, own_tile), KEY_TILE, 0)

    for extra in range(1, per_shard):
        tile(own_tile + extra, KEY_TILE, extra * KEY_TILE)
    for h in range(heads):
        o_ref[h] = (acc_ref[h] / sum_ref[h]).T.astype(o_ref.dtype)
        lse_ref[h] = max_ref[h] + jnp.log2(sum_ref[h])


def bwd_kernel(scale, meta_ref, start_ref, q_ref, do_ref, o_ref, lse_ref, k_ref, v_ref, dq_ref, dkv_ref, dqt_ref, delta_ref):
    heads, toks, dim = q_ref.shape
    per_shard = toks // KEY_TILE
    own_tile = meta_ref[1]
    q_first = own_tile * KEY_TILE
    coef = scale * LOG2E

    @pl.when(pl.program_id(1) == 0)
    def _():
        dkv_ref[...] = jnp.zeros_like(dkv_ref)

    dqt_ref[...] = jnp.zeros_like(dqt_ref)
    for h in range(heads):
        prod = do_ref[h].astype(jnp.float32) * o_ref[h].astype(jnp.float32)
        delta_ref[h] = jnp.sum(prod.T, axis=0, keepdims=True)

    def tile(index, lo):
        shard = index // per_shard
        row = pl.multiple_of((index % per_shard) * KEY_TILE, KEY_TILE)
        rows = pl.ds(row, KEY_TILE)
        keys = k_ref[shard, 0, 0, rows, :]
        keys_t = keys.T
        vals = v_ref[shard, 0, 0, rows, :]
        query_pos = q_first + lo + lax.broadcasted_iota(jnp.int32, (1, toks - lo), 1)
        bias = tile_bias(index * KEY_TILE, KEY_TILE, start_ref[:, lo:], query_pos)
        dk = jnp.zeros((KEY_TILE, dim), jnp.float32)
        dv = jnp.zeros((KEY_TILE, dim), jnp.float32)
        for h in range(heads):
            q_h = q_ref[h, lo:, :]
            do_h = do_ref[h, lo:, :]
            scores = dot32(keys, q_h, NT) * coef + bias
            prob = jnp.exp2(scores - lse_ref[h, :, lo:])
            dprob = dot32(vals, do_h, NT)
            dscore = (prob * (dprob - delta_ref[h, :, lo:])).astype(jnp.bfloat16)
            dv = dv + dot32(prob.astype(jnp.bfloat16), do_h, NN)
            dk = dk + dot32(dscore, q_h, NN)
            dqt_ref[h, :, lo:] += dot32(keys_t, dscore, NN)
        dkv_ref[shard, 0, 0, rows, :] += dk
        dkv_ref[shard, 0, 1, rows, :] += dv

    @pl.loop(meta_ref[0], own_tile + 1)
    def _(index):
        tile(index, 0)

    for extra in range(1, per_shard):
        tile(own_tile + extra, extra * KEY_TILE)
    for h in range(heads):
        dq_ref[h] = (dqt_ref[h] * scale).T.astype(dq_ref.dtype)


def tail_kernel(scale, kv_heads, ring, x_ref, gq_ref, dkvp_ref, o_ref, ol_ref, or_ref, dy0_ref, dy1_ref, dy2_ref, dy3_ref,
                dwq_ref, dwk_ref, dwv_ref, dkv_ref, dwo_ref, oo_ref, dyt_ref, o_buf, o_far, o_sems, xp_ref, gqp_ref, xt_ref, w_buf, d_buf, dp_buf, v_buf, bufb_ref, bufp_ref,
                d_load, pair_send, pair_recv, ring_send, ring_recv):
    n = 2 * ring
    idx = lax.axis_index('cp')
    core, chip = idx % 2, idx // 2
    partner = idx + 1 - 2 * core
    hop = ((idx + 2) % n, (idx + n - 2) % n)
    toks, model = x_ref.shape
    heads, _, dim = gq_ref.shape
    rows = model // n
    wide = w_buf.shape[-1]
    per = wide // dim
    parts = w_buf.shape[1]

    def target(way, step):
        return (chip + ring - 1 - step) % ring if way == 0 else (chip + 1 + step) % ring

    barrier = pltpu.get_barrier_semaphore()
    for other in (partner, *hop):
        pl.semaphore_signal(barrier, inc=1, device_id={'cp': other}, device_id_type=pl.DeviceIdType.MESH)

    loads = [[pltpu.make_async_copy(dkvp_ref.at[2 * target(way, step) + core, way], d_buf.at[way, step] if step == 0 else dp_buf.at[1, way, step - 1],
                                    d_load.at[way, step]) for way in range(2)] for step in range(ring)]
    for row in loads:
        for copy in row:
            copy.start()
    pl.semaphore_wait(barrier, 3)

    def to_partner(src, dst, slot):
        return pltpu.make_async_remote_copy(src_ref=src, dst_ref=dst, send_sem=pair_send.at[slot], recv_sem=pair_recv.at[slot],
                                            device_id={'cp': partner}, device_id_type=pl.DeviceIdType.MESH)

    d_pair = [[to_partner(dkvp_ref.at[2 * target(way, step) + 1 - core, way], dp_first(dp_buf, way, step), 2 * step + way)
               for way in range(2)] for step in range(ring)]
    base = 2 * ring
    x_pair = [to_partner(x_ref.at[:, pl.ds(pl.multiple_of((2 * t + 1 - core) * rows, rows), rows)], xp_ref.at[t], base + t) for t in range(ring)]
    q_pair = to_partner(gq_ref, gqp_ref, base + ring)
    b_pair = to_partner(bufb_ref, bufp_ref, base + ring + 1)
    half, quarter = heads // 2, heads // 4

    def o_hop(way, part):
        where = pl.ds(way * half + part * quarter, quarter)
        return pltpu.make_async_remote_copy(src_ref=(ol_ref, or_ref)[way].at[where], dst_ref=oo_ref.at[where],
                                            send_sem=o_sems.at[0, way, part], recv_sem=o_sems.at[1, way, part],
                                            device_id={'cp': hop[way]}, device_id_type=pl.DeviceIdType.MESH)

    def o_pair(way, part):
        where = pl.ds((way * half + part * quarter) // 2, quarter // 2)
        return pltpu.make_async_remote_copy(src_ref=o_buf.at[1 - core, where], dst_ref=o_far.at[where],
                                            send_sem=o_sems.at[2, way, part], recv_sem=o_sems.at[3, way, part],
                                            device_id={'cp': partner}, device_id_type=pl.DeviceIdType.MESH)

    for way in range(2):
        o_hop(way, 0).start()
    for copy in d_pair[0] + x_pair + [q_pair]:
        copy.start()
    for row in d_pair[1:]:
        for copy in row:
            copy.start()

    class Job:
        def __init__(self, buf, slot, add):
            self.buf, self.slot, self.contribution = buf, slot, add

        def copy(self, way, step):
            return pltpu.make_async_remote_copy(src_ref=self.buf.at[way, step], dst_ref=self.buf.at[way, step + 1],
                                                send_sem=ring_send.at[self.slot, way, step], recv_sem=ring_recv.at[self.slot, way, step],
                                                device_id={'cp': hop[way]}, device_id_type=pl.DeviceIdType.MESH)

        def add(self, step):
            for way in range(2):
                if step:
                    self.copy(way, step - 1).wait_recv()
                self.contribution(way, step)

        def send(self, step):
            for way in range(2):
                self.copy(way, step).start()

        def drain(self):
            for step in range(ring - 1):
                for way in range(2):
                    self.copy(way, step).wait_send()

    def d_add(way, step):
        loads[step][way].wait()
        d_pair[step][way].wait_recv()
        if step == 0:
            d_buf[way, 0] += dp_buf[0, way, 0]
        else:
            d_buf[way, step] += dp_buf[1, way, step - 1] + dp_first(dp_buf, way, step)[...]

    def w_add(part):
        def add(way, step):
            t = target(way, step)
            first = (way * parts + part) * per

            def product(pair):
                h = first + 2 * pair
                own = jnp.concatenate([gq_ref[h], gq_ref[h + 1]], axis=1)
                far = jnp.concatenate([gqp_ref[h], gqp_ref[h + 1]], axis=1)
                return dot32(xt_ref[t, :, :toks], own, NN) + dot32(xt_ref[t, :, toks:], far, NN)

            if step < ring - 1:
                @pl.loop(0, per // 2)
                def _(pair):
                    cols = pl.ds(pl.multiple_of(2 * pair * dim, 2 * dim), 2 * dim)
                    if step == 0:
                        w_buf[way, part, 0, :, cols] = product(pair)
                    else:
                        w_buf[way, part, step, :, cols] += product(pair)
            else:
                for pair in range(per // 2):
                    total = w_buf[way, part, step, :, 2 * pair * dim:2 * (pair + 1) * dim] + product(pair)
                    dwq_ref[:, first + 2 * pair, :] = total[:, :dim]
                    dwq_ref[:, first + 2 * pair + 1, :] = total[:, dim:]
        return add

    def v_add(way, step):
        t = target(way, step)
        own = jnp.concatenate([bufb_ref[way, g] for g in range(kv_heads)], axis=1)
        far = jnp.concatenate([bufp_ref[way, g] for g in range(kv_heads)], axis=1)
        part_sum = dot32(xt_ref[t, :, :toks], own, NN) + dot32(xt_ref[t, :, toks:], far, NN)
        if step == 0:
            v_buf[way, 0] = part_sum
        elif step < ring - 1:
            v_buf[way, step] += part_sum
        else:
            total = v_buf[way, step] + part_sum
            for g in range(kv_heads):
                (dwk_ref, dwv_ref)[way][:, g, :] = total[:, g * dim:(g + 1) * dim]

    class Part:
        def __init__(self, part):
            self.part = part

        @property
        def at(self):
            part = self.part

            class View:
                def __getitem__(self, key):
                    return w_buf.at[key[0], part, key[1]]
            return View()

    d_job = Job(d_buf, 0, d_add)
    v_job = Job(v_buf, 1, v_add)
    w_jobs = [Job(Part(part), 2 + part, w_add(part)) for part in range(parts)]

    d_job.add(0)
    d_job.send(0)
    for way in range(2):
        o_hop(way, 1).start()
    for t in range(ring):
        own_cols = pl.ds(pl.multiple_of((2 * t + core) * rows, rows), rows)
        xt_ref[t, :, :toks] = x_ref[:, own_cols].T
    for t in range(ring):
        x_pair[t].wait_recv()
        xt_ref[t, :, toks:] = xp_ref[t].T
    q_pair.wait_recv()
    w0, w1 = w_jobs
    w0.add(0)
    w0.send(0)
    d_job.add(1)
    d_job.send(1)
    w1.add(0)
    w1.send(0)
    for i, ref in enumerate((dy0_ref, dy1_ref, dy2_ref, dy3_ref)):
        dyt_ref[i] = ref[...].T

    @pl.loop(0, half)
    def _(pair):
        total = jnp.zeros((2 * rows, 2 * dim), jnp.float32)
        for i, ref in enumerate((o_ref, ol_ref, or_ref)):
            total += dot32(dyt_ref[i], jnp.concatenate([ref[2 * pair], ref[2 * pair + 1]], axis=1), NN)
        o_buf[0, pair] = total[:rows]
        o_buf[1, pair] = total[rows:]

    d_job.add(2)
    d_job.send(2)
    for job in w_jobs:
        job.add(1)
        job.send(1)
    for part in range(2):
        for way in range(2):
            o_hop(way, part).wait_recv()

            @pl.loop((way * half + part * quarter) // 2, (way * half + part * quarter + quarter) // 2)
            def _(pair):
                total = dot32(dyt_ref[3], jnp.concatenate([oo_ref[2 * pair], oo_ref[2 * pair + 1]], axis=1), NN)
                o_buf[0, pair] += total[:rows]
                o_buf[1, pair] += total[rows:]
    d_job.add(ring - 1)
    for part in range(2):
        for way in range(2):
            o_pair(way, part).start()
    for g in range(kv_heads):
        bufb_ref[0, g] = (d_buf[g, ring - 1, 0] * scale).astype(bufb_ref.dtype)
        bufb_ref[1, g] = d_buf[g, ring - 1, 1].astype(bufb_ref.dtype)
    dkv_ref[...] = bufb_ref[...]
    b_pair.start()
    b_pair.wait_recv()
    v_job.add(0)
    v_job.send(0)
    for part in range(2):
        for way in range(2):
            o_pair(way, part).wait_recv()
            for pair in range((way * half + part * quarter) // 2, (way * half + part * quarter + quarter) // 2):
                total = o_buf[core, pair] + o_far[pair]
                dwo_ref[:, 2 * pair, :] = total[:, :dim]
                dwo_ref[:, 2 * pair + 1, :] = total[:, dim:]
    w0.add(2)
    w0.send(2)
    v_job.add(1)
    v_job.send(1)
    w1.add(2)
    w1.send(2)
    v_job.add(2)
    v_job.send(2)
    w0.add(3)
    w1.add(3)
    v_job.add(3)
    for copy in [*x_pair, q_pair, b_pair, *sum(d_pair, [])]:
        copy.wait_send()
    for part in range(2):
        for way in range(2):
            o_hop(way, part).wait_send()
            o_pair(way, part).wait_send()
    for job in (d_job, v_job, *w_jobs):
        job.drain()


def dp_first(dp_buf, way, step):
    return dp_buf.at[0, way, step]


def tail_reduce(x_act, grad_q, dkv_part, o_blocks, dy_blocks, scale):
    n, kv_heads, _, toks, dim = dkv_part.shape
    heads, model = grad_q.shape[0], x_act.shape[1]
    ring, rows, parts = n // 2, x_act.shape[1] // n, 2
    wide = heads * dim // (2 * parts)
    bf16, f32 = jnp.bfloat16, jnp.float32
    vmem = pl.BlockSpec(memory_space=pltpu.VMEM)
    n_pair = 3 * ring + 2
    return pl.pallas_call(
        functools.partial(tail_kernel, scale, kv_heads, ring),
        in_specs=[vmem, vmem, pl.BlockSpec(memory_space=pl.ANY)] + [vmem] * 7,
        out_specs=[vmem] * 5,
        out_shape=[jax.ShapeDtypeStruct((rows, heads, dim), f32)] + [jax.ShapeDtypeStruct((rows, kv_heads, dim), f32)] * 2 + [
                   jax.ShapeDtypeStruct((2, kv_heads, toks, dim), bf16), jax.ShapeDtypeStruct((rows, heads, dim), f32)],
        scratch_shapes=[
            pltpu.VMEM((heads, toks, dim), bf16), pltpu.VMEM((ring, 2 * rows, toks), bf16),
            pltpu.VMEM((2, heads // 2, rows, 2 * dim), f32), pltpu.VMEM((heads // 2, rows, 2 * dim), f32), pltpu.SemaphoreType.DMA((4, 2, 2)),
            pltpu.VMEM((ring, toks, rows), bf16), pltpu.VMEM((heads, toks, dim), bf16), pltpu.VMEM((ring, rows, 2 * toks), bf16),
            pltpu.VMEM((2, parts, ring, rows, wide), f32), pltpu.VMEM((2, ring, 2, toks, dim), f32),
            pltpu.VMEM((2, 2, ring, 2, toks, dim), f32), pltpu.VMEM((2, ring, rows, kv_heads * dim), f32),
            pltpu.VMEM((2, kv_heads, toks, dim), bf16), pltpu.VMEM((2, kv_heads, toks, dim), bf16),
            pltpu.SemaphoreType.DMA((2, ring)), pltpu.SemaphoreType.DMA((n_pair,)), pltpu.SemaphoreType.DMA((n_pair,)),
            pltpu.SemaphoreType.DMA((2 + parts, 2, ring - 1)), pltpu.SemaphoreType.DMA((2 + parts, 2, ring - 1))],
        compiler_params=pltpu.CompilerParams(collective_id=0, has_side_effects=True, vmem_limit_bytes=62 * 2 ** 20),
        cost_estimate=pl.CostEstimate(flops=2 * 10 ** 11, bytes_accessed=2 ** 24, transcendentals=0),
        name='tail_reduce',
    )(x_act, grad_q, dkv_part, *o_blocks, *dy_blocks)


def gather_kernel(n, kv_ref, seg_ref, all_ref, segs_ref, seg_sems, ring_sems, mate_sems):
    idx = lax.axis_index('cp')
    partner = idx + 1 - 2 * (idx % 2)
    right, left, opposite = (idx + 2) % n, (idx + n - 2) % n, (idx + n // 2) % n
    mesh_id = pl.DeviceIdType.MESH
    barrier = pltpu.get_barrier_semaphore()
    for off in range(1, n):
        pl.semaphore_signal(barrier, inc=1, device_id={'cp': (idx + off) % n}, device_id_type=mesh_id)
    segs_ref[idx] = seg_ref[...]
    pl.semaphore_wait(barrier, n - 1)

    def remote(src, dst, sems, slot, device):
        return pltpu.make_async_remote_copy(src_ref=src, dst_ref=dst, send_sem=sems.at[0, slot], recv_sem=sems.at[1, slot],
                                            device_id={'cp': device}, device_id_type=mesh_id)

    own = [[remote(kv_ref.at[g], all_ref.at[idx, g], ring_sems, 3 * way + i, (right, left)[way])
            for i, g in enumerate(((0, 1), (1, 0))[way])] for way in range(2)]
    onward = [remote(all_ref.at[(left, right)[way], way], all_ref.at[(left, right)[way], way], ring_sems, 3 * way + 2, (right, left)[way])
              for way in range(2)]
    mine = remote(kv_ref, all_ref.at[idx], mate_sems, 0, partner)
    shares = [[remote(all_ref.at[(left, right)[way], g], all_ref.at[(left, right)[way], g], mate_sems, 1 + 2 * way + i, partner)
               for i, g in enumerate(((0, 1), (1, 0))[way])] for way in range(2)]
    far_shares = [remote(all_ref.at[opposite, way], all_ref.at[opposite, way], mate_sems, 5 + way, partner) for way in range(2)]
    segs = [remote(seg_ref, segs_ref.at[idx], seg_sems, off - 1, (idx + off) % n) for off in range(1, n)]
    for i in range(2):
        for way in range(2):
            own[way][i].start()
    for copy in segs:
        copy.start()
    mine.start()
    all_ref[idx] = kv_ref[...]
    for way in range(2):
        own[way][0].wait_recv()
        onward[way].start()
        shares[way][0].start()
    for way in range(2):
        own[way][1].wait_recv()
        shares[way][1].start()
    for way in range(2):
        onward[way].wait_recv()
        far_shares[way].start()
    for copy in segs + [mine] + shares[0] + shares[1] + far_shares:
        copy.wait()
    for copy in own[0] + own[1] + onward:
        copy.wait_send()


def gather_keys(kv_loc, seg_ids, n):
    vmem = pl.BlockSpec(memory_space=pltpu.VMEM)
    kv_all, segs = pl.pallas_call(
        functools.partial(gather_kernel, n), in_specs=[vmem, vmem], out_specs=[vmem, vmem],
        out_shape=[jax.ShapeDtypeStruct((n, *kv_loc.shape), kv_loc.dtype), jax.ShapeDtypeStruct((n, seg_ids.shape[0] // 128, 128), jnp.int32)],
        scratch_shapes=[pltpu.SemaphoreType.DMA((2, n - 1)), pltpu.SemaphoreType.DMA((2, 6)), pltpu.SemaphoreType.DMA((2, 7))],
        compiler_params=pltpu.CompilerParams(collective_id=1, has_side_effects=True, vmem_limit_bytes=16 * 2 ** 20),
        cost_estimate=pl.CostEstimate(flops=2 * 10 ** 10, bytes_accessed=2 ** 22, transcendentals=0),
        name='gather_keys',
    )(kv_loc, seg_ids.reshape(-1, 128))
    return kv_all, segs.reshape(-1)


def solution(mesh):
    group_count = mesh.shape['cp']
    row_spec = P(('dp', 'cp'), None)
    tok_spec = P(('dp', 'cp'))
    weight_spec = P(None, None, None)
    grad_spec = P(('dp', 'cp'), None, None)

    def local_step(x_act, seg_ids, w_q, w_k, w_v, w_o, dy_act):
        toks = x_act.shape[0]
        model_dim, q_heads, dim = w_q.shape
        kv_heads = w_k.shape[1]
        group = q_heads // kv_heads
        halves = group // HEAD_UNROLL
        scale = dim ** -0.5
        my_index = lax.axis_index('cp')
        bf16, f32 = jnp.bfloat16, jnp.float32

        k_loc = jnp.einsum('sm,mkd->ksd', x_act, w_k, preferred_element_type=f32).astype(bf16)
        v_loc = jnp.einsum('sm,mkd->ksd', x_act, w_v, preferred_element_type=f32).astype(bf16)
        up = [(i, (i + 2) % group_count) for i in range(group_count)]
        down = [(i, (i - 2) % group_count) for i in range(group_count)]
        far = [(i, (i + group_count // 2) % group_count) for i in range(group_count)]

        def move(value, pairs):
            return lax.ppermute(value, 'cp', pairs)

        kv_loc = jnp.stack([k_loc, v_loc], axis=1)
        kv_all, seg_all = gather_keys(kv_loc, seg_ids, group_count)
        chip = my_index // 2
        ring = group_count // 2
        chip_rows = model_dim // ring
        dy_gate, kv_gate, seg_all = lax.optimization_barrier((dy_act, kv_all, seg_all))

        def dy_cols(dist):
            return lax.dynamic_slice_in_dim(dy_gate, ((chip + dist) % ring) * chip_rows, chip_rows, 1)

        dy_blocks = [dy_cols(0), move(dy_cols(1), up), move(dy_cols(ring - 1), down), move(dy_cols(ring // 2), far)]
        q_loc = jnp.einsum('sm,mhd->hsd', x_act, w_q, preferred_element_type=f32).astype(bf16)
        doc_start = jnp.sum((seg_all[None, :] < seg_ids[:, None]).astype(jnp.int32), axis=1)
        meta = jnp.stack([doc_start[0] // KEY_TILE, my_index * (toks // KEY_TILE)]).astype(jnp.int32)
        start_row = doc_start[None, :]

        grid = (kv_heads, halves)
        head_spec = pl.BlockSpec((HEAD_UNROLL, toks, dim), lambda g, b, m: (g * halves + b, 0, 0))
        stat_spec = pl.BlockSpec((HEAD_UNROLL, 1, toks), lambda g, b, m: (g * halves + b, 0, 0))
        start_spec = pl.BlockSpec((1, toks), lambda g, b, m: (0, 0))
        key_spec, val_spec = (pl.BlockSpec((group_count, 1, 1, toks, dim), lambda g, b, m, i=i: (0, g, i, 0, 0)) for i in range(2))
        tile_flops = 2 * q_heads * toks * toks * dim * 3
        o_loc, lse = pl.pallas_call(
            functools.partial(fwd_kernel, scale),
            grid_spec=pltpu.PrefetchScalarGridSpec(
                num_scalar_prefetch=1, grid=grid,
                in_specs=[start_spec, head_spec, key_spec, val_spec],
                out_specs=[head_spec, stat_spec],
                scratch_shapes=[pltpu.VMEM((HEAD_UNROLL, dim, toks), f32), pltpu.VMEM((HEAD_UNROLL, 1, toks), f32),
                                pltpu.VMEM((HEAD_UNROLL, 1, toks), f32)]),
            out_shape=[jax.ShapeDtypeStruct((q_heads, toks, dim), bf16), jax.ShapeDtypeStruct((q_heads, 1, toks), f32)],
            compiler_params=pltpu.CompilerParams(dimension_semantics=('arbitrary', 'arbitrary'), vmem_limit_bytes=56 * 2 ** 20),
            cost_estimate=pl.CostEstimate(flops=tile_flops * 2, bytes_accessed=2 ** 23, transcendentals=0),
            name='attn_fwd',
        )(meta, start_row, q_loc, kv_gate, kv_gate)

        o_loc, dy_late, *dy_blocks = lax.optimization_barrier((o_loc, dy_act, *dy_blocks))
        o_blocks = [o_loc, move(o_loc, up), move(o_loc, down)]
        do_loc = jnp.einsum('qm,mhd->hqd', dy_late, w_o, preferred_element_type=f32).astype(bf16)
        y_out = jnp.einsum('hqd,mhd->qm', o_loc, w_o, preferred_element_type=f32).astype(bf16)

        grid = (kv_heads, group // BWD_UNROLL)
        head_spec = pl.BlockSpec((BWD_UNROLL, toks, dim), lambda g, b, m: (g * (group // BWD_UNROLL) + b, 0, 0))
        stat_spec = pl.BlockSpec((BWD_UNROLL, 1, toks), lambda g, b, m: (g * (group // BWD_UNROLL) + b, 0, 0))
        grad_q, dkv_part = pl.pallas_call(
            functools.partial(bwd_kernel, scale),
            grid_spec=pltpu.PrefetchScalarGridSpec(
                num_scalar_prefetch=1, grid=grid,
                in_specs=[start_spec, head_spec, head_spec, head_spec, stat_spec, key_spec, val_spec],
                out_specs=[head_spec, pl.BlockSpec((group_count, 1, 2, toks, dim), lambda g, b, m: (0, g, 0, 0, 0))],
                scratch_shapes=[pltpu.VMEM((BWD_UNROLL, dim, toks), f32), pltpu.VMEM((BWD_UNROLL, 1, toks), f32)]),
            out_shape=[jax.ShapeDtypeStruct((q_heads, toks, dim), bf16),
                       jax.ShapeDtypeStruct((group_count, kv_heads, 2, toks, dim), f32)],
            compiler_params=pltpu.CompilerParams(dimension_semantics=('arbitrary', 'arbitrary'), vmem_limit_bytes=60 * 2 ** 20),
            cost_estimate=pl.CostEstimate(flops=tile_flops * 5, bytes_accessed=2 ** 24, transcendentals=0),
            name='attn_bwd',
        )(meta, start_row, q_loc, do_loc, o_loc, lse, kv_gate, kv_gate)

        dx_query = jnp.einsum('hqd,mhd->qm', grad_q, w_q, preferred_element_type=f32)
        grad_q, dkv_part, y_out, dx_query = lax.optimization_barrier((grad_q, dkv_part, y_out, dx_query))
        dwq, dwk, dwv, grad_kv, dwo = tail_reduce(x_act, grad_q, dkv_part, o_blocks, dy_blocks, scale)
        dx_wide = (dx_query + jnp.einsum('ksd,mkd->sm', grad_kv[0], w_k, preferred_element_type=f32)
                   + jnp.einsum('ksd,mkd->sm', grad_kv[1], w_v, preferred_element_type=f32))
        return y_out, dx_wide.astype(bf16), dwq, dwk, dwv, dwo

    return jax.shard_map(local_step, mesh=mesh,
                         in_specs=(row_spec, tok_spec, weight_spec, weight_spec, weight_spec, weight_spec, row_spec),
                         out_specs=(row_spec, row_spec, grad_spec, grad_spec, grad_spec, grad_spec),
                         check_vma=False)
```

```python
import functools
import jax
import jax.numpy as jnp
from jax import lax
from jax.experimental import pallas as pl
from jax.experimental.pallas import tpu as pltpu
from jax.sharding import PartitionSpec as P

LOG2E = 1.4426950408889634
NEG_START = -1e30
KEY_TILE = 256
HEAD_UNROLL = 4
BWD_UNROLL = 8
ROW_BLOCK = 32
NT = (((1,), (1,)), ((), ()))
NN = (((1,), (0,)), ((), ()))


def dot32(a, b, dims):
    return lax.dot_general(a, b, dims, preferred_element_type=jnp.float32)


def tile_bias(first_key, n_keys, doc_start, query_pos):
    key_pos = first_key + lax.broadcasted_iota(jnp.int32, (n_keys, doc_start.shape[1]), 0)
    allowed = (key_pos >= doc_start) & (key_pos <= query_pos)
    return jnp.where(allowed, 0.0, -jnp.inf)


def fwd_kernel(scale, meta_ref, start_ref, q_ref, k_ref, v_ref, o_ref, lse_ref, acc_ref, max_ref, sum_ref):
    heads, toks, dim = q_ref.shape
    per_shard = toks // KEY_TILE
    own_tile = meta_ref[1]
    q_first = own_tile * KEY_TILE
    acc_ref[...] = jnp.zeros_like(acc_ref)
    max_ref[...] = jnp.full_like(max_ref, NEG_START)
    sum_ref[...] = jnp.zeros_like(sum_ref)
    coef = scale * LOG2E

    def tile(index, size, lo):
        shard = index // per_shard
        row = pl.multiple_of((index % per_shard) * KEY_TILE, KEY_TILE)
        keys = k_ref[shard, 0, 0, pl.ds(row, size), :]
        vals_t = v_ref[shard, 0, 0, pl.ds(row, size), :].T
        query_pos = q_first + lo + lax.broadcasted_iota(jnp.int32, (1, toks - lo), 1)
        bias = tile_bias(index * KEY_TILE, size, start_ref[:, lo:], query_pos)
        for h in range(heads):
            scores = dot32(keys, q_ref[h, lo:, :], NT) * coef + bias
            old_max = max_ref[h, :, lo:]
            new_max = jnp.maximum(old_max, jnp.max(scores, axis=0, keepdims=True))
            weights = jnp.exp2(scores - new_max)
            factor = jnp.exp2(old_max - new_max)
            max_ref[h, :, lo:] = new_max
            sum_ref[h, :, lo:] = sum_ref[h, :, lo:] * factor + jnp.sum(weights, axis=0, keepdims=True)
            acc_ref[h, :, lo:] = acc_ref[h, :, lo:] * factor + dot32(vals_t, weights.astype(jnp.bfloat16), NN)

    first_tile = meta_ref[0]
    odd = jnp.where(first_tile < own_tile, first_tile % per_shard, 0)

    @pl.loop((first_tile + odd) // per_shard, own_tile // per_shard)
    def _(shard):
        tile(shard * per_shard, per_shard * KEY_TILE, 0)

    @pl.loop(0, odd + 1)
    def _(i):
        tile(jnp.where(i < odd, first_tile, own_tile), KEY_TILE, 0)

    for extra in range(1, per_shard):
        tile(own_tile + extra, KEY_TILE, extra * KEY_TILE)
    for h in range(heads):
        o_ref[h] = (acc_ref[h] / sum_ref[h]).T.astype(o_ref.dtype)
        lse_ref[h] = max_ref[h] + jnp.log2(sum_ref[h])


def bwd_kernel(scale, meta_ref, start_ref, q_ref, do_ref, o_ref, lse_ref, k_ref, v_ref, dq_ref, dkv_ref, dqt_ref, delta_ref):
    heads, toks, dim = q_ref.shape
    per_shard = toks // KEY_TILE
    own_tile = meta_ref[1]
    q_first = own_tile * KEY_TILE
    coef = scale * LOG2E

    @pl.when(pl.program_id(1) == 0)
    def _():
        dkv_ref[...] = jnp.zeros_like(dkv_ref)

    dqt_ref[...] = jnp.zeros_like(dqt_ref)
    for h in range(heads):
        prod = do_ref[h].astype(jnp.float32) * o_ref[h].astype(jnp.float32)
        delta_ref[h] = jnp.sum(prod.T, axis=0, keepdims=True)

    def tile(index, lo):
        shard = index // per_shard
        row = pl.multiple_of((index % per_shard) * KEY_TILE, KEY_TILE)
        rows = pl.ds(row, KEY_TILE)
        keys = k_ref[shard, 0, 0, rows, :]
        keys_t = keys.T
        vals = v_ref[shard, 0, 0, rows, :]
        query_pos = q_first + lo + lax.broadcasted_iota(jnp.int32, (1, toks - lo), 1)
        bias = tile_bias(index * KEY_TILE, KEY_TILE, start_ref[:, lo:], query_pos)
        dk = jnp.zeros((KEY_TILE, dim), jnp.float32)
        dv = jnp.zeros((KEY_TILE, dim), jnp.float32)
        for h in range(heads):
            q_h = q_ref[h, lo:, :]
            do_h = do_ref[h, lo:, :]
            scores = dot32(keys, q_h, NT) * coef + bias
            prob = jnp.exp2(scores - lse_ref[h, :, lo:])
            dprob = dot32(vals, do_h, NT)
            dscore = (prob * (dprob - delta_ref[h, :, lo:])).astype(jnp.bfloat16)
            dv = dv + dot32(prob.astype(jnp.bfloat16), do_h, NN)
            dk = dk + dot32(dscore, q_h, NN)
            dqt_ref[h, :, lo:] += dot32(keys_t, dscore, NN)
        dkv_ref[shard, 0, 0, rows, :] += dk
        dkv_ref[shard, 0, 1, rows, :] += dv

    @pl.loop(meta_ref[0], own_tile + 1)
    def _(index):
        tile(index, 0)

    for extra in range(1, per_shard):
        tile(own_tile + extra, extra * KEY_TILE)
    for h in range(heads):
        dq_ref[h] = (dqt_ref[h] * scale).T.astype(dq_ref.dtype)


def tail_kernel(scale, kv_heads, ring, x_ref, gq_ref, dkvp_ref, o_ref, ol_ref, or_ref, dy0_ref, dy1_ref, dy2_ref, dy3_ref, wq_ref, wo_ref, wk_ref, wv_ref,
                dwq_ref, dwk_ref, dwv_ref, dwo_ref, y_ref, dx_ref, w_chunk, wk_chunk, w_flat, w_sems, oo_ref, dyt_ref, o_buf, o_far, o_sems, xp_ref, gqp_ref, xt_ref, w_buf, d_buf, dp_buf, d_own, v_buf, bufb_ref, bufp_ref,
                d_load, pair_send, pair_recv, ring_send, ring_recv):
    n = 2 * ring
    idx = lax.axis_index('cp')
    core, chip = idx % 2, idx // 2
    partner = idx + 1 - 2 * core
    hop = ((idx + 2) % n, (idx + n - 2) % n)
    toks, model = x_ref.shape
    heads, _, dim = gq_ref.shape
    rows = model // n
    wide = w_buf.shape[-1]
    per = wide // dim
    parts = w_buf.shape[1]

    def target(way, step):
        return (chip + ring - 1 - step) % ring if way == 0 else (chip + 1 + step) % ring

    barrier = pltpu.get_barrier_semaphore()
    for other in (partner, *hop):
        pl.semaphore_signal(barrier, inc=1, device_id={'cp': other}, device_id_type=pl.DeviceIdType.MESH)

    loads = [[pltpu.make_async_copy(dkvp_ref.at[2 * target(way, step) + core, way], d_buf.at[way, 0] if step == 0 else d_own.at[way],
                                    d_load.at[way, step]) for way in range(2)] for step in range(ring)]
    for row in loads[:2]:
        for copy in row:
            copy.start()
    pl.semaphore_wait(barrier, 3)

    def to_partner(src, dst, slot):
        return pltpu.make_async_remote_copy(src_ref=src, dst_ref=dst, send_sem=pair_send.at[slot], recv_sem=pair_recv.at[slot],
                                            device_id={'cp': partner}, device_id_type=pl.DeviceIdType.MESH)

    d_pair = [[to_partner(dkvp_ref.at[2 * target(way, step) + 1 - core, way], dp_buf.at[way, step], 2 * step + way)
               for way in range(2)] for step in range(ring)]
    base = 2 * ring
    x_pair = [to_partner(x_ref.at[:, pl.ds(pl.multiple_of((2 * t + 1 - core) * rows, rows), rows)], xp_ref.at[t], base + t) for t in range(ring)]
    q_pair = to_partner(gq_ref, gqp_ref, base + ring)
    b_pair = to_partner(bufb_ref, bufp_ref, base + ring + 1)
    half, quarter = heads // 2, heads // 4

    def o_hop(way, part):
        where = pl.ds(way * half + part * quarter, quarter)
        return pltpu.make_async_remote_copy(src_ref=(ol_ref, or_ref)[way].at[where], dst_ref=oo_ref.at[where],
                                            send_sem=o_sems.at[0, way, part], recv_sem=o_sems.at[1, way, part],
                                            device_id={'cp': hop[way]}, device_id_type=pl.DeviceIdType.MESH)

    def o_pair(way, part):
        where = pl.ds((way * half + part * quarter) // 2, quarter // 2)
        return pltpu.make_async_remote_copy(src_ref=o_buf.at[1 - core, where], dst_ref=o_far.at[where],
                                            send_sem=o_sems.at[2, way, part], recv_sem=o_sems.at[3, way, part],
                                            device_id={'cp': partner}, device_id_type=pl.DeviceIdType.MESH)

    for way in range(2):
        o_hop(way, 0).start()
    for copy in d_pair[0] + x_pair + [q_pair]:
        copy.start()
    for row in d_pair[1:]:
        for copy in row:
            copy.start()

    class Job:
        def __init__(self, buf, slot, add):
            self.buf, self.slot, self.contribution = buf, slot, add

        def copy(self, way, step):
            return pltpu.make_async_remote_copy(src_ref=self.buf.at[way, step], dst_ref=self.buf.at[way, step + 1],
                                                send_sem=ring_send.at[self.slot, way, step], recv_sem=ring_recv.at[self.slot, way, step],
                                                device_id={'cp': hop[way]}, device_id_type=pl.DeviceIdType.MESH)

        def add(self, step):
            for way in range(2):
                if step:
                    self.copy(way, step - 1).wait_recv()
                self.contribution(way, step)

        def send(self, step):
            for way in range(2):
                self.copy(way, step).start()

        def drain(self):
            for step in range(ring - 1):
                for way in range(2):
                    self.copy(way, step).wait_send()

    def d_add(way, step):
        loads[step][way].wait()
        d_pair[step][way].wait_recv()
        if step == 0:
            d_buf[way, 0] += dp_buf[way, 0]
        else:
            d_buf[way, step] += d_own[way] + dp_buf[way, step]
            if step + 1 < ring:
                loads[step + 1][way].start()

    def w_add(part):
        def add(way, step):
            t = target(way, step)
            first = (way * parts + part) * per

            def product(pair):
                h = first + 2 * pair
                own = jnp.concatenate([gq_ref[h], gq_ref[h + 1]], axis=1)
                far = jnp.concatenate([gqp_ref[h], gqp_ref[h + 1]], axis=1)
                return dot32(xt_ref[t, :, :toks], own, NN) + dot32(xt_ref[t, :, toks:], far, NN)

            if step < ring - 1:
                @pl.loop(0, per // 2)
                def _(pair):
                    cols = pl.ds(pl.multiple_of(2 * pair * dim, 2 * dim), 2 * dim)
                    if step == 0:
                        w_buf[way, part, 0, :, cols] = product(pair)
                    else:
                        w_buf[way, part, step, :, cols] += product(pair)
            else:
                for pair in range(per // 2):
                    total = w_buf[way, part, step, :, 2 * pair * dim:2 * (pair + 1) * dim] + product(pair)
                    dwq_ref[:, first + 2 * pair, :] = total[:, :dim]
                    dwq_ref[:, first + 2 * pair + 1, :] = total[:, dim:]
        return add

    def v_add(way, step):
        t = target(way, step)
        own = jnp.concatenate([bufb_ref[way, g] for g in range(kv_heads)], axis=1)
        far = jnp.concatenate([bufp_ref[way, g] for g in range(kv_heads)], axis=1)
        part_sum = dot32(xt_ref[t, :, :toks], own, NN) + dot32(xt_ref[t, :, toks:], far, NN)
        if step == 0:
            v_buf[way, 0] = part_sum
        elif step < ring - 1:
            v_buf[way, step] += part_sum
        else:
            total = v_buf[way, step] + part_sum
            for g in range(kv_heads):
                (dwk_ref, dwv_ref)[way][:, g, :] = total[:, g * dim:(g + 1) * dim]

    class Part:
        def __init__(self, part):
            self.part = part

        @property
        def at(self):
            part = self.part

            class View:
                def __getitem__(self, key):
                    return w_buf.at[key[0], part, key[1]]
            return View()

    d_job = Job(d_buf, 0, d_add)
    v_job = Job(v_buf, 1, v_add)
    w_jobs = [Job(Part(part), 2 + part, w_add(part)) for part in range(parts)]

    def fetch(weights, i, slot):
        block = pl.ds(pl.multiple_of(i * rows, rows), rows)
        copies = [pltpu.make_async_copy(weights.at[block], w_chunk.at[slot], w_sems.at[0, slot])]
        if weights is wq_ref:
            copies += [pltpu.make_async_copy(ref.at[block], wk_chunk.at[c, slot], w_sems.at[1 + c, slot]) for c, ref in enumerate((wk_ref, wv_ref))]
        return copies

    def project(weights, lhs_ref, out_ref):
        for copy in fetch(weights, 0, 0):
            copy.start()

        @pl.loop(0, n)
        def _(i):
            for copy in fetch(weights, i, 0):
                copy.wait()

            @pl.loop(0, rows // ROW_BLOCK)
            def _(b):
                some = pl.ds(pl.multiple_of(b * ROW_BLOCK, ROW_BLOCK), ROW_BLOCK)
                for h in range(heads):
                    w_flat[some, h * dim:(h + 1) * dim] = w_chunk[0, some, h, :]

            lhs = [lhs_ref[h] for h in range(heads)]
            width = heads * dim
            if weights is wq_ref:
                for c in range(2):
                    for g in range(kv_heads):
                        w_flat[:, width:width + dim] = wk_chunk[c, 0, :, g, :]
                        lhs.append(bufb_ref[c, g])
                        width += dim

            @pl.when(i + 1 < n)
            def _():
                for copy in fetch(weights, i + 1, 0):
                    copy.start()

            total = jnp.zeros((toks, rows), jnp.float32)
            for h in range(0, len(lhs), 4):
                total += dot32(jnp.concatenate(lhs[h:h + 4], axis=1), w_flat[:, h * dim:(h + 4) * dim], NT)
            out_ref[:, pl.ds(pl.multiple_of(i * rows, rows), rows)] = total.astype(out_ref.dtype)

    d_job.add(0)
    d_job.send(0)
    for way in range(2):
        o_hop(way, 1).start()
    for t in range(ring):
        @pl.loop(0, rows // 128)
        def _(c):
            some = pl.ds(pl.multiple_of(c * 128, 128), 128)
            xt_ref[t, some, :toks] = x_ref[:, pl.ds(pl.multiple_of((2 * t + core) * rows + c * 128, 128), 128)].T

    for t in range(ring):
        x_pair[t].wait_recv()

        @pl.loop(0, rows // 128)
        def _(c):
            some = pl.ds(pl.multiple_of(c * 128, 128), 128)
            xt_ref[t, some, toks:] = xp_ref[t, :, some].T

    q_pair.wait_recv()
    w0, w1 = w_jobs
    w0.add(0)
    w0.send(0)
    d_job.add(1)
    d_job.send(1)
    w1.add(0)
    w1.send(0)
    for i, ref in enumerate((dy0_ref, dy1_ref, dy2_ref, dy3_ref)):
        @pl.loop(0, 2 * rows // 128)
        def _(c):
            some = pl.ds(pl.multiple_of(c * 128, 128), 128)
            dyt_ref[i, some, :] = ref[:, some].T


    @pl.loop(0, half)
    def _(pair):
        total = jnp.zeros((2 * rows, 2 * dim), jnp.float32)
        for i, ref in enumerate((o_ref, ol_ref, or_ref)):
            total += dot32(dyt_ref[i], jnp.concatenate([ref[2 * pair], ref[2 * pair + 1]], axis=1), NN)
        o_buf[0, pair] = total[:rows]
        o_buf[1, pair] = total[rows:]

    project(wo_ref, o_ref, y_ref)
    d_job.add(2)
    d_job.send(2)
    for job in w_jobs:
        job.add(1)
        job.send(1)
    for part in range(2):
        for way in range(2):
            o_hop(way, part).wait_recv()

            @pl.loop((way * half + part * quarter) // 2, (way * half + part * quarter + quarter) // 2)
            def _(pair):
                total = dot32(dyt_ref[3], jnp.concatenate([oo_ref[2 * pair], oo_ref[2 * pair + 1]], axis=1), NN)
                o_buf[0, pair] += total[:rows]
                o_buf[1, pair] += total[rows:]
    d_job.add(ring - 1)
    for part in range(2):
        for way in range(2):
            o_pair(way, part).start()
    for g in range(kv_heads):
        bufb_ref[0, g] = (d_buf[g, ring - 1, 0] * scale).astype(bufb_ref.dtype)
        bufb_ref[1, g] = d_buf[g, ring - 1, 1].astype(bufb_ref.dtype)
    b_pair.start()
    b_pair.wait_recv()
    v_job.add(0)
    v_job.send(0)
    for part in range(2):
        for way in range(2):
            o_pair(way, part).wait_recv()
            for pair in range((way * half + part * quarter) // 2, (way * half + part * quarter + quarter) // 2):
                total = o_buf[core, pair] + o_far[pair]
                dwo_ref[:, 2 * pair, :] = total[:, :dim]
                dwo_ref[:, 2 * pair + 1, :] = total[:, dim:]
    project(wq_ref, gq_ref, dx_ref)
    w0.add(2)
    w0.send(2)
    v_job.add(1)
    v_job.send(1)
    w1.add(2)
    w1.send(2)
    v_job.add(2)
    v_job.send(2)
    w0.add(3)
    w1.add(3)
    v_job.add(3)
    for copy in [*x_pair, q_pair, b_pair, *sum(d_pair, [])]:
        copy.wait_send()
    for part in range(2):
        for way in range(2):
            o_hop(way, part).wait_send()
            o_pair(way, part).wait_send()
    for job in (d_job, v_job, *w_jobs):
        job.drain()


def tail_reduce(x_act, grad_q, dkv_part, o_blocks, dy_blocks, weights, scale):
    n, kv_heads, _, toks, dim = dkv_part.shape
    heads, model = grad_q.shape[0], x_act.shape[1]
    ring, rows, parts = n // 2, x_act.shape[1] // n, 2
    wide = heads * dim // (2 * parts)
    bf16, f32 = jnp.bfloat16, jnp.float32
    vmem = pl.BlockSpec(memory_space=pltpu.VMEM)
    n_pair = 3 * ring + 2
    return pl.pallas_call(
        functools.partial(tail_kernel, scale, kv_heads, ring),
        in_specs=[vmem, vmem, pl.BlockSpec(memory_space=pl.ANY)] + [vmem] * 7 + [pl.BlockSpec(memory_space=pl.ANY)] * 4,
        out_specs=[vmem] * 6,
        out_shape=[jax.ShapeDtypeStruct((rows, heads, dim), f32)] + [jax.ShapeDtypeStruct((rows, kv_heads, dim), f32)] * 2 + [
                   jax.ShapeDtypeStruct((rows, heads, dim), f32)] + [jax.ShapeDtypeStruct((toks, model), bf16)] * 2,
        scratch_shapes=[
            pltpu.VMEM((1, rows, heads, dim), bf16), pltpu.VMEM((2, 1, rows, kv_heads, dim), bf16),
            pltpu.VMEM((rows, (heads + 2 * kv_heads) * dim), bf16), pltpu.SemaphoreType.DMA((3, 2)),
            pltpu.VMEM((heads, toks, dim), bf16), pltpu.VMEM((ring, 2 * rows, toks), bf16),
            pltpu.VMEM((2, heads // 2, rows, 2 * dim), f32), pltpu.VMEM((heads // 2, rows, 2 * dim), f32), pltpu.SemaphoreType.DMA((4, 2, 2)),
            pltpu.VMEM((ring, toks, rows), bf16), pltpu.VMEM((heads, toks, dim), bf16), pltpu.VMEM((ring, rows, 2 * toks), bf16),
            pltpu.VMEM((2, parts, ring, rows, wide), f32), pltpu.VMEM((2, ring, 2, toks, dim), f32),
            pltpu.VMEM((2, ring, 2, toks, dim), f32), pltpu.VMEM((2, 2, toks, dim), f32), pltpu.VMEM((2, ring, rows, kv_heads * dim), f32),
            pltpu.VMEM((2, kv_heads, toks, dim), bf16), pltpu.VMEM((2, kv_heads, toks, dim), bf16),
            pltpu.SemaphoreType.DMA((2, ring)), pltpu.SemaphoreType.DMA((n_pair,)), pltpu.SemaphoreType.DMA((n_pair,)),
            pltpu.SemaphoreType.DMA((2 + parts, 2, ring - 1)), pltpu.SemaphoreType.DMA((2 + parts, 2, ring - 1))],
        compiler_params=pltpu.CompilerParams(collective_id=0, has_side_effects=True, vmem_limit_bytes=67043328),
        cost_estimate=pl.CostEstimate(flops=2 * 10 ** 11, bytes_accessed=2 ** 24, transcendentals=0),
        name='tail_reduce',
    )(x_act, grad_q, dkv_part, *o_blocks, *dy_blocks, *weights)


def gather_kernel(n, kv_ref, seg_ref, x_ref, wq_ref, all_ref, segs_ref, q_ref, w_chunk, w_flat, acc_ref, w_sems, seg_sems, ring_sems, mate_sems):
    idx = lax.axis_index('cp')
    partner = idx + 1 - 2 * (idx % 2)
    right, left, opposite = (idx + 2) % n, (idx + n - 2) % n, (idx + n // 2) % n
    mesh_id = pl.DeviceIdType.MESH
    barrier = pltpu.get_barrier_semaphore()
    for off in range(1, n):
        pl.semaphore_signal(barrier, inc=1, device_id={'cp': (idx + off) % n}, device_id_type=mesh_id)
    segs_ref[idx] = seg_ref[...]

    def fetch(i, slot):
        block = pl.ds(pl.multiple_of(i * w_flat.shape[0], w_flat.shape[0]), w_flat.shape[0])
        return pltpu.make_async_copy(wq_ref.at[block], w_chunk.at[slot], w_sems.at[slot])

    fetch(0, 0).start()
    pl.semaphore_wait(barrier, n - 1)

    def remote(src, dst, sems, slot, device):
        return pltpu.make_async_remote_copy(src_ref=src, dst_ref=dst, send_sem=sems.at[0, slot], recv_sem=sems.at[1, slot],
                                            device_id={'cp': device}, device_id_type=mesh_id)

    own = [[remote(kv_ref.at[g], all_ref.at[idx, g], ring_sems, 3 * way + i, (right, left)[way])
            for i, g in enumerate(((0, 1), (1, 0))[way])] for way in range(2)]
    onward = [remote(all_ref.at[(left, right)[way], way], all_ref.at[(left, right)[way], way], ring_sems, 3 * way + 2, (right, left)[way])
              for way in range(2)]
    mine = remote(kv_ref, all_ref.at[idx], mate_sems, 0, partner)
    shares = [[remote(all_ref.at[(left, right)[way], g], all_ref.at[(left, right)[way], g], mate_sems, 1 + 2 * way + i, partner)
               for i, g in enumerate(((0, 1), (1, 0))[way])] for way in range(2)]
    far_shares = [remote(all_ref.at[opposite, way], all_ref.at[opposite, way], mate_sems, 5 + way, partner) for way in range(2)]
    segs = [remote(seg_ref, segs_ref.at[idx], seg_sems, off - 1, (idx + off) % n) for off in range(1, n)]
    for i in range(2):
        for way in range(2):
            own[way][i].start()
    for copy in segs:
        copy.start()
    mine.start()
    all_ref[idx] = kv_ref[...]
    heads, _, dim = q_ref.shape
    rows = w_flat.shape[0]
    acc_ref[...] = jnp.zeros_like(acc_ref)

    @pl.loop(0, n)
    def _(i):
        slot = i % 2
        fetch(i, slot).wait()

        @pl.when(i + 1 < n)
        def _():
            fetch(i + 1, 1 - slot).start()

        @pl.when(i == n // 2)
        def _():
            for way in range(2):
                own[way][0].wait_recv()
                onward[way].start()
                shares[way][0].start()

        @pl.loop(0, rows // ROW_BLOCK)
        def _(b):
            some = pl.ds(pl.multiple_of(b * ROW_BLOCK, ROW_BLOCK), ROW_BLOCK)
            for h in range(heads):
                w_flat[some, h * dim:(h + 1) * dim] = w_chunk[slot, some, h, :]

        x_cols = x_ref[:, pl.ds(pl.multiple_of(i * rows, rows), rows)]
        for h in range(0, heads, 4):
            cols = slice(h * dim, (h + 4) * dim)
            acc_ref[:, cols] += dot32(x_cols, w_flat[:, cols], NN)

    for h in range(heads):
        q_ref[h] = acc_ref[:, h * dim:(h + 1) * dim].astype(q_ref.dtype)
    for way in range(2):
        own[way][1].wait_recv()
        shares[way][1].start()
    for way in range(2):
        onward[way].wait_recv()
        far_shares[way].start()
    for copy in segs + [mine] + shares[0] + shares[1] + far_shares:
        copy.wait()
    for copy in own[0] + own[1] + onward:
        copy.wait_send()


def gather_keys(kv_loc, seg_ids, x_act, w_q, n):
    vmem = pl.BlockSpec(memory_space=pltpu.VMEM)
    model, heads, dim = w_q.shape
    rows, toks = model // n, x_act.shape[0]
    kv_all, segs, q_loc = pl.pallas_call(
        functools.partial(gather_kernel, n), in_specs=[vmem, vmem, vmem, pl.BlockSpec(memory_space=pl.ANY)], out_specs=[vmem] * 3,
        out_shape=[jax.ShapeDtypeStruct((n, *kv_loc.shape), kv_loc.dtype), jax.ShapeDtypeStruct((n, seg_ids.shape[0] // 128, 128), jnp.int32),
                   jax.ShapeDtypeStruct((heads, toks, dim), x_act.dtype)],
        scratch_shapes=[pltpu.VMEM((2, rows, heads, dim), w_q.dtype), pltpu.VMEM((rows, heads * dim), w_q.dtype),
                        pltpu.VMEM((toks, heads * dim), jnp.float32), pltpu.SemaphoreType.DMA((2,)),
                        pltpu.SemaphoreType.DMA((2, n - 1)), pltpu.SemaphoreType.DMA((2, 6)), pltpu.SemaphoreType.DMA((2, 7))],
        compiler_params=pltpu.CompilerParams(collective_id=1, has_side_effects=True, vmem_limit_bytes=28 * 2 ** 20),
        cost_estimate=pl.CostEstimate(flops=2 * 10 ** 10, bytes_accessed=2 ** 22, transcendentals=0),
        name='gather_keys',
    )(kv_loc, seg_ids.reshape(-1, 128), x_act, w_q)
    return kv_all, segs.reshape(-1), q_loc


def solution(mesh):
    group_count = mesh.shape['cp']
    row_spec = P(('dp', 'cp'), None)
    tok_spec = P(('dp', 'cp'))
    weight_spec = P(None, None, None)
    grad_spec = P(('dp', 'cp'), None, None)

    def local_step(x_act, seg_ids, w_q, w_k, w_v, w_o, dy_act):
        toks = x_act.shape[0]
        model_dim, q_heads, dim = w_q.shape
        kv_heads = w_k.shape[1]
        group = q_heads // kv_heads
        halves = group // HEAD_UNROLL
        scale = dim ** -0.5
        my_index = lax.axis_index('cp')
        bf16, f32 = jnp.bfloat16, jnp.float32

        k_loc = jnp.einsum('sm,mkd->ksd', x_act, w_k, preferred_element_type=f32).astype(bf16)
        v_loc = jnp.einsum('sm,mkd->ksd', x_act, w_v, preferred_element_type=f32).astype(bf16)
        up = [(i, (i + 2) % group_count) for i in range(group_count)]
        down = [(i, (i - 2) % group_count) for i in range(group_count)]
        far = [(i, (i + group_count // 2) % group_count) for i in range(group_count)]

        def move(value, pairs):
            return lax.ppermute(value, 'cp', pairs)

        kv_loc = jnp.stack([k_loc, v_loc], axis=1)
        kv_all, seg_all, q_loc = gather_keys(kv_loc, seg_ids, x_act, w_q, group_count)
        chip = my_index // 2
        ring = group_count // 2
        chip_rows = model_dim // ring
        dy_gate, kv_gate, seg_all = lax.optimization_barrier((dy_act, kv_all, seg_all))

        def dy_cols(dist):
            return lax.dynamic_slice_in_dim(dy_gate, ((chip + dist) % ring) * chip_rows, chip_rows, 1)

        dy_blocks = [dy_cols(0), move(dy_cols(1), up), move(dy_cols(ring - 1), down), move(dy_cols(ring // 2), far)]
        doc_start = jnp.sum((seg_all[None, :] < seg_ids[:, None]).astype(jnp.int32), axis=1)
        meta = jnp.stack([doc_start[0] // KEY_TILE, my_index * (toks // KEY_TILE)]).astype(jnp.int32)
        start_row = doc_start[None, :]

        grid = (kv_heads, halves)
        head_spec = pl.BlockSpec((HEAD_UNROLL, toks, dim), lambda g, b, m: (g * halves + b, 0, 0))
        stat_spec = pl.BlockSpec((HEAD_UNROLL, 1, toks), lambda g, b, m: (g * halves + b, 0, 0))
        start_spec = pl.BlockSpec((1, toks), lambda g, b, m: (0, 0))
        key_spec, val_spec = (pl.BlockSpec((group_count, 1, 1, toks, dim), lambda g, b, m, i=i: (0, g, i, 0, 0)) for i in range(2))
        tile_flops = 2 * q_heads * toks * toks * dim * 3
        o_loc, lse = pl.pallas_call(
            functools.partial(fwd_kernel, scale),
            grid_spec=pltpu.PrefetchScalarGridSpec(
                num_scalar_prefetch=1, grid=grid,
                in_specs=[start_spec, head_spec, key_spec, val_spec],
                out_specs=[head_spec, stat_spec],
                scratch_shapes=[pltpu.VMEM((HEAD_UNROLL, dim, toks), f32), pltpu.VMEM((HEAD_UNROLL, 1, toks), f32),
                                pltpu.VMEM((HEAD_UNROLL, 1, toks), f32)]),
            out_shape=[jax.ShapeDtypeStruct((q_heads, toks, dim), bf16), jax.ShapeDtypeStruct((q_heads, 1, toks), f32)],
            compiler_params=pltpu.CompilerParams(dimension_semantics=('arbitrary', 'arbitrary'), vmem_limit_bytes=56 * 2 ** 20),
            cost_estimate=pl.CostEstimate(flops=tile_flops * 2, bytes_accessed=2 ** 23, transcendentals=0),
            name='attn_fwd',
        )(meta, start_row, q_loc, kv_gate, kv_gate)

        o_loc, dy_late, *dy_blocks = lax.optimization_barrier((o_loc, dy_act, *dy_blocks))
        o_blocks = [o_loc, move(o_loc, up), move(o_loc, down)]
        do_loc = jnp.einsum('qm,mhd->hqd', dy_late, w_o, preferred_element_type=f32).astype(bf16)
        grid = (kv_heads, group // BWD_UNROLL)
        head_spec = pl.BlockSpec((BWD_UNROLL, toks, dim), lambda g, b, m: (g * (group // BWD_UNROLL) + b, 0, 0))
        stat_spec = pl.BlockSpec((BWD_UNROLL, 1, toks), lambda g, b, m: (g * (group // BWD_UNROLL) + b, 0, 0))
        grad_q, dkv_part = pl.pallas_call(
            functools.partial(bwd_kernel, scale),
            grid_spec=pltpu.PrefetchScalarGridSpec(
                num_scalar_prefetch=1, grid=grid,
                in_specs=[start_spec, head_spec, head_spec, head_spec, stat_spec, key_spec, val_spec],
                out_specs=[head_spec, pl.BlockSpec((group_count, 1, 2, toks, dim), lambda g, b, m: (0, g, 0, 0, 0))],
                scratch_shapes=[pltpu.VMEM((BWD_UNROLL, dim, toks), f32), pltpu.VMEM((BWD_UNROLL, 1, toks), f32)]),
            out_shape=[jax.ShapeDtypeStruct((q_heads, toks, dim), bf16),
                       jax.ShapeDtypeStruct((group_count, kv_heads, 2, toks, dim), f32)],
            compiler_params=pltpu.CompilerParams(dimension_semantics=('arbitrary', 'arbitrary'), vmem_limit_bytes=60 * 2 ** 20),
            cost_estimate=pl.CostEstimate(flops=tile_flops * 5, bytes_accessed=2 ** 24, transcendentals=0),
            name='attn_bwd',
        )(meta, start_row, q_loc, do_loc, o_loc, lse, kv_gate, kv_gate)

        dwq, dwk, dwv, dwo, y_out, dx_out = tail_reduce(x_act, grad_q, dkv_part, o_blocks, dy_blocks, (w_q, w_o, w_k, w_v), scale)
        return y_out, dx_out, dwq, dwk, dwv, dwo

    return jax.shard_map(local_step, mesh=mesh,
                         in_specs=(row_spec, tok_spec, weight_spec, weight_spec, weight_spec, weight_spec, row_spec),
                         out_specs=(row_spec, row_spec, grad_spec, grad_spec, grad_spec, grad_spec),
                         check_vma=False)
```
